32 devices in a mesh: gx: 4 (over z), gy: 4 (over y, x), gz: 2 (over core).
Axes of the slice: x: 2, y: 2, z: 4, core: 2. Of those that a mesh axis runs over, the one named last changes fastest.
Arguments:
- field: bfloat16 [32, 32, 32, 256], P(None, 'gx', 'gy', 'gz'), may hold values from -6 to 6
- mixing: bfloat16 [32, 32], replicated, may hold values from -1 to 1
- kernel_fine: bfloat16 [3, 3, 3, 32, 32], replicated, may hold values from -0.21875 to 0.21875
- kernel_half: bfloat16 [3, 3, 3, 32, 32], replicated, may hold values from -1.5 to 1.5
- kernel_quarter: bfloat16 [3, 3, 3, 32, 32], replicated, may hold values from -4 to 4
- kernel_eighth: bfloat16 [3, 3, 3, 32, 32], replicated, may hold values from -6 to 6
Outputs:
- layer_out: bfloat16 [32, 32, 32, 256], P(None, 'gx', 'gy', 'gz')
The draws below stay inside these ranges and needn't reach their ends.
All inputs are finite; a program needn't handle non-finite values.
Results may differ from the reference program's by a relative error of at most 0.008.
Values may be sent and summed in bfloat16 or wider, within the bound.
A program may use at most 128 MiB of HBM per device.

```python
import jax
import jax.numpy as jnp
from jax import lax

C = 32
NX = 32
NY = 32
NZ = 256


def level_of(rng, shape, shards, low, largest):
    def one(dim, blocks):
        draws = jax.random.uniform(jax.random.fold_in(jax.random.fold_in(rng, 6), dim), (blocks,), jnp.float32, low / len(shards), largest / len(shards))
        return jnp.repeat(jnp.exp(draws), shape[dim] // blocks).reshape((-1,) + (1,) * (len(shape) - dim - 1))

    factor_of = one(*shards[0])
    for cut in shards[1:]:
        factor_of = factor_of * one(*cut)
    return factor_of


def noise(own_key, dims, deviation, bound, pieces=(), held_as=jnp.bfloat16):
    level = level_of(own_key, dims, pieces, -0.22, 0.18) if pieces else 1.0
    drawn = jax.random.normal(own_key, dims, jnp.float32) * deviation * level
    return jnp.minimum(jnp.maximum(drawn, -bound), bound).astype(held_as)


def setup_inputs(seed: int = 0) -> dict:
    seeds = jax.random.split(jax.random.key(seed), 7)
    field = noise(seeds[0], (C, NX, NY, NZ), 1.0, 6.0, ((1, 4), (2, 4), (3, 2)))
    mixing = noise(seeds[1], (C, C), C ** -0.5, 1.0)
    kernel_fine = noise(seeds[2], (3, 3, 3, C, C), (27 * C) ** -0.5, 0.21875)
    kernel_half = noise(seeds[3], (3, 3, 3, C, C), (3 * (27 * C) ** -0.5), 1.5)
    kernel_quarter = noise(seeds[4], (3, 3, 3, C, C), (9 * (27 * C) ** -0.5), 4.0)
    kernel_eighth = noise(seeds[5], (3, 3, 3, C, C), (27 * (27 * C) ** -0.5), 6.0)
    return dict(field=field, mixing=mixing, kernel_fine=kernel_fine, kernel_half=kernel_half, kernel_quarter=kernel_quarter, kernel_eighth=kernel_eighth)


def restrict(values):
    chans, sizex, sizey, sizez = values.shape
    blocks = values.astype(jnp.float32).reshape(chans, sizex // 2, 2, sizey // 2, 2, sizez // 2, 2)
    return jnp.mean(blocks, axis=(2, 4, 6)).astype(jnp.bfloat16)


def kernel_apply(values, kernel):
    result = lax.conv_general_dilated(values[None], kernel, (1, 1, 1), ((1, 1), (1, 1), (1, 1)),
                                      dimension_numbers=("NCDHW", "DHWIO", "NCDHW"),
                                      preferred_element_type=jnp.float32)
    return result[0]


def refine_padded(padded, dimension):
    length = padded.shape[dimension]
    inner = lax.slice_in_dim(padded, 1, length - 1, axis=dimension)
    lower = lax.slice_in_dim(padded, 0, length - 2, axis=dimension)
    upper = lax.slice_in_dim(padded, 2, length, axis=dimension)
    even_cells = 0.75 * inner + 0.25 * lower
    odd_cells = 0.75 * inner + 0.25 * upper
    joined = jnp.stack([even_cells, odd_cells], axis=dimension + 1)
    shape_out = list(inner.shape)
    shape_out[dimension] = shape_out[dimension] * 2
    return joined.reshape(shape_out)


def prolong(values):
    current = values.astype(jnp.float32)
    for dimension in (1, 2, 3):
        widths = [(0, 0)] * 4
        widths[dimension] = (1, 1)
        current = refine_padded(jnp.pad(current, widths), dimension)
    return current


def reference(field, mixing, kernel_fine, kernel_half, kernel_quarter, kernel_eighth):
    kernels = (kernel_fine, kernel_half, kernel_quarter, kernel_eighth)
    levels_list = [field]
    for depth in range(3):
        levels_list.append(restrict(levels_list[-1]))
    outputs = [kernel_apply(levels_list[depth], kernels[depth]) for depth in range(4)]
    carried = outputs[3].astype(jnp.bfloat16)
    for depth in (2, 1):
        carried = (outputs[depth] + prolong(carried)).astype(jnp.bfloat16)
    chans = field.shape[0]
    mixed = jnp.dot(mixing, field.reshape(chans, -1), preferred_element_type=jnp.float32).reshape(field.shape)
    total = mixed + outputs[0] + prolong(carried)
    return jax.nn.gelu(total, approximate=True).astype(jnp.bfloat16)
```

```python
import functools
import math

import jax
import jax.numpy as jnp
from jax import lax
from jax.experimental import pallas as pl
from jax.experimental.pallas import tpu as pltpu
from jax.sharding import PartitionSpec as P

F32 = jnp.float32
BF16 = jnp.bfloat16
MESH = pl.DeviceIdType.MESH


def iota(shape, dim):
    return lax.broadcasted_iota(jnp.int32, shape, dim)


def pair_sum(first, offset, lanes):
    source, target = iota((lanes, lanes), 0) - first, iota((lanes, lanes), 1) - offset
    return jnp.where(
        (source >= 0) & (target >= 0) & (lax.shift_right_arithmetic(source, 1) == target), 1.0, 0.0
    )


def spread(coarse_size, fine_shift, lanes):
    coarse = iota((lanes, lanes), 0) - 1
    fine = iota((lanes, lanes), 1) - fine_shift
    main = lax.shift_right_arithmetic(fine, 1)
    other = main + 2 * (fine & 1) - 1
    weight = jnp.where(coarse == main, 0.75, jnp.where(coarse == other, 0.25, 0.0))
    return jnp.where(coarse <= coarse_size, weight, 0.0).astype(BF16)


def dot(a, b):
    return jnp.dot(a, b, preferred_element_type=F32)


def kernel(counts, field, w0, wc, out, u0, uc, u3x, u3y, z0, zc, z3, v0, v1, v2, v3,
           zz1, zz2, zz3, qy0, send, recv):
    chans, bx, by, bz = field.shape
    cx, cy, cz = bx // 2, by // 2, bz // 2
    nx, ny, nz = counts
    gx, gy, gz = lax.axis_index("gx"), lax.axis_index("gy"), lax.axis_index("gz")
    place = {"gx": gx, "gy": gy, "gz": gz}
    size = {"gx": nx, "gy": ny, "gz": nz}
    reach = [("gx", d) for d in (-1, 1, -2, 2)] + [("gy", d) for d in (-1, 1, -2, 2)]
    reach += [("gz", -1), ("gz", 1)]

    def has(axis, d):
        target = place[axis] + d
        return (target >= 0) & (target < size[axis])

    def device(axis, d):
        where = dict(place)
        where[axis] = jnp.clip(place[axis] + d, 0, size[axis] - 1)
        return (where["gx"], where["gy"], where["gz"])

    for ref in (u0, uc, u3x, u3y, z0, zc, z3):
        ref[...] = jnp.zeros_like(ref)

    barrier = pltpu.get_barrier_semaphore()
    for axis, d in reach:
        if size[axis] > abs(d):
            @pl.when(has(axis, d))
            def _():
                pl.semaphore_signal(barrier, inc=1, device_id=device(axis, d), device_id_type=MESH)

    rows = chans * by
    perm_row, perm_col = iota((rows, rows), 0), iota((rows, rows), 1)
    perm = jnp.where(perm_col == (perm_row % chans) * by + perm_row // chans, 1.0, 0.0).astype(BF16)
    back = jnp.where(perm_row == (perm_col % chans) * by + perm_col // chans, 1.0, 0.0).astype(BF16)

    for x in range(bx):
        slab = field[:, x].astype(F32).reshape(rows, bz).astype(BF16)
        u0[1 + x, 1 : 1 + by] = dot(perm, slab).astype(BF16).reshape(by, chans, bz)

    def halve(blocks, matrix):
        stacked = jnp.concatenate(blocks, axis=0)
        summed = jnp.dot(stacked, matrix, precision=lax.Precision.HIGHEST, preferred_element_type=F32)
        rounded = (summed * 0.125).astype(BF16).astype(F32)
        return [rounded[chans * k : chans * (k + 1)] for k in range(len(blocks))]

    def quads(values, wide, high):
        return [
            values[2 * x * high + 2 * y] + values[(2 * x + 1) * high + 2 * y]
            + values[2 * x * high + 2 * y + 1] + values[(2 * x + 1) * high + 2 * y + 1]
            for x in range(wide // 2) for y in range(high // 2)
        ]

    fine = [u0[1 + x, 1 + y].astype(F32) for x in range(bx) for y in range(by)]
    first = halve(quads(fine, bx, by), pair_sum(0, 0, bz))
    second = halve(quads(first, cx, cy), pair_sum(0, cz, bz))
    third = halve(quads(second, cx // 2, cy // 2), pair_sum(cz, 0, bz))
    for x in range(cx):
        for y in range(cy):
            uc[2 + x, 2 + y] = (first[x * cy + y] + second[(x % 2) * (cy // 2) + y % 2]).astype(BF16)
    u3x[2] = third[0].astype(BF16)

    peers = sum(has(axis, d).astype(jnp.int32) for axis, d in reach)
    pl.semaphore_wait(barrier, peers)

    made = []

    def copy(axis, d, src, dst):
        k = len(made)
        made.append((axis, d))
        return axis, d, pltpu.make_async_remote_copy(
            src_ref=src, dst_ref=dst, send_sem=send.at[k], recv_sem=recv.at[k],
            device_id=device(axis, d), device_id_type=MESH)

    def start(copies):
        for axis, d, c in copies:
            if size[axis] > abs(d):
                @pl.when(has(axis, d))
                def _():
                    c.start()

    def arrive(copies):
        for axis, d, c in copies:
            if size[axis] > abs(d):
                @pl.when(has(axis, -d))
                def _():
                    c.wait_recv()

    def leave(copies):
        for axis, d, c in copies:
            if size[axis] > abs(d):
                @pl.when(has(axis, d))
                def _():
                    c.wait_send()

    own_y, own_cy = pl.ds(1, by), pl.ds(2, cy)
    x_small = [
        copy("gx", -1, uc.at[pl.ds(2, 2), own_cy], uc.at[pl.ds(cx + 2, 2), own_cy]),
        copy("gx", 1, uc.at[pl.ds(cx, 2), own_cy], uc.at[pl.ds(0, 2), own_cy]),
    ] + [copy("gx", d, u3x.at[2], u3x.at[2 - d]) for d in (-1, 1, -2, 2)]
    x_fine = [
        copy("gx", -1, u0.at[1, own_y], u0.at[bx + 1, own_y]),
        copy("gx", 1, u0.at[bx, own_y], u0.at[0, own_y]),
    ]
    y_small = [
        copy("gy", -1, uc.at[:, pl.ds(2, 2)], uc.at[:, pl.ds(cy + 2, 2)]),
        copy("gy", 1, uc.at[:, pl.ds(cy, 2)], uc.at[:, pl.ds(0, 2)]),
    ] + [copy("gy", d, u3y.at[2], u3y.at[2 - d]) for d in (-1, 1, -2, 2)]
    y_fine = [
        copy("gy", -1, u0.at[:, pl.ds(1, 1)], u0.at[:, pl.ds(by + 1, 1)]),
        copy("gy", 1, u0.at[:, pl.ds(by, 1)], u0.at[:, pl.ds(0, 1)]),
    ]
    z_small = [
        copy("gz", d, src, dst.at[(1 - d) // 2]) for d in (-1, 1) for src, dst in ((uc, zc), (u3y, z3))
    ]
    z_fine = [copy("gz", d, u0, z0.at[(1 - d) // 2]) for d in (-1, 1)]

    start(x_small)
    start(x_fine)
    arrive(x_small)
    width = bz // 8
    packed = u3x[0].astype(F32)
    for k in range(1, 5):
        packed = packed + pltpu.roll(u3x[k].astype(F32), k * width, 1)
    u3y[2] = packed.astype(BF16)
    start(y_small)
    arrive(x_fine)
    start(y_fine)
    arrive(y_small)
    start(z_small)
    arrive(y_fine)
    start(z_fine)
    arrive(z_small)

    lane = iota((chans, bz), 1)

    def roll(value, amount):
        amount = amount % bz
        return value if amount == 0 else pltpu.roll(value, amount, 1)

    def window(own, low, high, offset, length):
        own, low, high = own.astype(F32), low.astype(F32), high.astype(F32)
        value = jnp.where(lane < 2, roll(low, 2 - offset - length), 0.0)
        value = jnp.where((lane >= 2) & (lane < length + 2), roll(own, 2 - offset), value)
        value = jnp.where((lane >= length + 2) & (lane < length + 4), roll(high, length + 2 - offset), value)
        return jnp.concatenate([roll(value, -dz) for dz in range(3)], axis=0).astype(BF16)

    for k in range(5):
        for y in range(5):
            v3[k, y] = window(u3y[y], z3[0, y], z3[1, y], k * width, width)

    def fill2(x, carry):
        source_x = jnp.where(x >= 4, x + 2, x)
        for y in range(6):
            sy = y + 2 if y >= 4 else y
            v2[x, y] = window(uc[source_x, sy], zc[0, source_x, sy], zc[1, source_x, sy], cz, cz // 2)
        return carry

    lax.fori_loop(0, 6, fill2, 0)

    def fill1(x, carry):
        for y in range(cy + 4):
            v1[x, y] = window(uc[x, y], zc[0, x, y], zc[1, x, y], 0, cz)
        return carry

    lax.fori_loop(0, cx + 4, fill1, 0)

    depth = wc.shape[2]

    def patches(v, x, y):
        return jnp.concatenate(
            [v[x + dx, pl.ds(y, 3)].reshape(depth // 3, bz) for dx in range(3)], axis=0)

    def rim(length):
        low = jnp.where(gz > 0, 1.0, 0.0)
        high = jnp.where(gz < nz - 1, 1.0, 0.0)
        inside = jnp.where((lane >= 1) & (lane <= length), 1.0, 0.0)
        return inside + jnp.where(lane == 0, low, 0.0) + jnp.where(lane == length + 1, high, 0.0)

    def inside(index, length, axis):
        low = (index > 0) | (place[axis] > 0)
        high = (index <= length) | (place[axis] < size[axis] - 1)
        return jnp.where(low & high, 1.0, 0.0)

    rim3 = rim(width)
    w3 = wc[2]
    for x in range(3):
        for y in range(3):
            value = dot(w3, patches(v3, x, y))
            scale = inside(x, 1, "gx") * inside(y, 1, "gy")
            zz3[x, y] = (value * (rim3 * scale)).astype(BF16)

    def along_y(values, wide, shift):
        result = []
        for f in range(wide):
            cell = f - shift
            main = (cell >> 1) + 1
            other = main + 1 if cell & 1 else main - 1
            result.append(0.75 * values[main] + 0.25 * values[other])
        return result

    def raised(zz, coarse_size, shift):
        count_x, count_y = zz.shape[:2]
        spread_z = spread(coarse_size, shift, bz)
        flat = dot(zz[...].reshape(count_x * count_y * chans, bz), spread_z)
        return flat.reshape(count_x, count_y, chans, bz)

    def level(weights, v, zz, coarse, size_x, size_y, length, qy):
        mask = rim(length)
        for i in range((size_x + 2) // 2):
            for y in range(size_y + 2):
                value = dot(weights, jnp.concatenate(
                    [patches(v, 2 * i, y), patches(v, 2 * i + 1, y)], axis=1))
                a, b = qy[i][y], qy[i + 1][y]
                scale = mask * inside(y, size_y, "gy")
                zz[2 * i, y] = ((value[:, :bz] + 0.75 * a + 0.25 * b)
                                * (scale * inside(2 * i, size_x, "gx"))).astype(BF16)
                zz[2 * i + 1, y] = ((value[:, bz:] + 0.75 * b + 0.25 * a)
                                    * (scale * inside(2 * i + 1, size_x, "gx"))).astype(BF16)

    q3 = raised(zz3, width, 1)
    qy3 = [along_y([q3[x, y] for y in range(3)], 4, 1) for x in range(3)]
    level(wc[1], v2, zz2, zz3, cx // 2, cy // 2, cz // 2, qy3)
    q2 = raised(zz2, cz // 2, 1)
    qy2 = [along_y([q2[x, y] for y in range(cy // 2 + 2)], cy + 2, 1) for x in range(cx // 2 + 2)]
    level(wc[0], v1, zz1, zz2, cx, cy, cz, qy2)
    q1 = raised(zz1, cz, 0)
    for x in range(cx + 2):
        for y, value in enumerate(along_y([q1[x, y] for y in range(cy + 2)], by, 0)):
            qy0[x, y] = value

    arrive(z_fine)

    def fill0(x, carry):
        for y in range(by + 2):
            own = u0[x, y]
            wide = own.astype(F32)
            low = jnp.where(lane == bz - 1, z0[0, x, y].astype(F32), wide)
            high = jnp.where(lane == 0, z0[1, x, y].astype(F32), wide)
            v0[x, y] = jnp.concatenate([roll(low, 1).astype(BF16), own, roll(high, -1).astype(BF16)], axis=0)
        return carry

    lax.fori_loop(0, bx + 2, fill0, 0)

    weights = w0[...]
    scale = math.sqrt(2.0 / math.pi)

    def finish(i, carry):
        done = []
        for y in range(by):
            sides = [
                jnp.concatenate([patches(v0, 2 * i + k, y), u0[2 * i + k + 1, y + 1]], axis=0)
                for k in range(2)
            ]
            value = dot(weights, jnp.concatenate(sides, axis=1))
            a, b, c = qy0[i, y], qy0[i + 1, y], qy0[i + 2, y]
            value = value + jnp.concatenate([0.75 * b + 0.25 * a, 0.75 * b + 0.25 * c], axis=1)
            inner = scale * (value + 0.044715 * (value * value * value))
            done.append((0.5 * value * (1.0 + jnp.tanh(inner))).astype(BF16))
        whole = dot(back, jnp.concatenate(done, axis=0))
        for k in range(2):
            part = whole[:, k * bz : (k + 1) * bz].reshape(chans, by, bz).astype(BF16)
            out[:, pl.ds(2 * i + k, 1)] = part.reshape(chans, 1, by, bz)
        return carry

    lax.fori_loop(0, bx // 2, finish, 0)

    for group in (x_small, x_fine, y_small, y_fine, z_small, z_fine):
        leave(group)


def solution(mesh):
    counts = tuple(mesh.shape[axis] for axis in ("gx", "gy", "gz"))

    def on_device(field, mixing, kernel_fine, kernel_half, kernel_quarter, kernel_eighth):
        chans, bx, by, bz = field.shape
        cx, cy = bx // 2, by // 2
        w0 = jnp.concatenate([kernel_fine.reshape(-1, chans), mixing.T], axis=0).T
        wc = jnp.stack([k.reshape(-1, chans) for k in (kernel_half, kernel_quarter, kernel_eighth)])
        wc = wc.transpose(0, 2, 1)
        vmem = pl.BlockSpec(memory_space=pltpu.VMEM)

        def buf(*dims, dtype=BF16):
            return pltpu.VMEM(dims, dtype)

        fine = (bx + 2, by + 2, chans, bz)
        coarse = (cx + 4, cy + 4, chans, bz)
        return pl.pallas_call(
            functools.partial(kernel, counts),
            out_shape=jax.ShapeDtypeStruct(field.shape, BF16),
            in_specs=[vmem] * 3,
            out_specs=vmem,
            scratch_shapes=[
                buf(*fine), buf(*coarse), buf(5, chans, bz), buf(5, chans, bz),
                buf(2, *fine), buf(2, *coarse), buf(2, 5, chans, bz),
                buf(bx + 2, by + 2, 3 * chans, bz),
                buf(cx + 4, cy + 4, 3 * chans, bz),
                buf(6, 6, 3 * chans, bz), buf(5, 5, 3 * chans, bz),
                buf(cx + 2, cy + 2, chans, bz), buf(4, 4, chans, bz), buf(3, 3, chans, bz),
                buf(cx + 2, by, chans, bz, dtype=F32),
                pltpu.SemaphoreType.DMA((22,)), pltpu.SemaphoreType.DMA((22,)),
            ],
            compiler_params=pltpu.CompilerParams(
                collective_id=0, has_side_effects=True, vmem_limit_bytes=56 * 2**20),
        )(field, w0, wc)

    placed = (P(None, "gx", "gy", "gz"), P(), P(), P(), P(), P())
    return jax.shard_map(
        on_device, mesh=mesh, in_specs=placed, out_specs=P(None, "gx", "gy", "gz"), check_vma=False
    )
```

```python
import functools
import math

import jax
import jax.numpy as jnp
from jax import lax
from jax.experimental import pallas as pl
from jax.experimental.pallas import tpu as pltpu
from jax.sharding import PartitionSpec as P

F32 = jnp.float32
BF16 = jnp.bfloat16
MESH = pl.DeviceIdType.MESH


def iota(shape, dim):
    return lax.broadcasted_iota(jnp.int32, shape, dim)


def pair_sum(first, offset, lanes):
    source, target = iota((lanes, lanes), 0) - first, iota((lanes, lanes), 1) - offset
    return jnp.where(
        (source >= 0) & (target >= 0) & (lax.shift_right_arithmetic(source, 1) == target), 1.0, 0.0
    )


def spread(coarse_size, fine_shift, lanes):
    coarse = iota((lanes, lanes), 0) - 1
    fine = iota((lanes, lanes), 1) - fine_shift
    main = lax.shift_right_arithmetic(fine, 1)
    other = main + 2 * (fine & 1) - 1
    weight = jnp.where(coarse == main, 0.75, jnp.where(coarse == other, 0.25, 0.0))
    return jnp.where(coarse <= coarse_size, weight, 0.0).astype(BF16)


def dot(a, b):
    return jnp.dot(a, b, preferred_element_type=F32)


def kernel(counts, field, mixing, raw_fine, raw_half, raw_quarter, raw_eighth, out, u0, uc, u3x, u3y,
           z0, zc, z3, v0, v1, v2, v3, zz1, zz2, zz3, qy0, y0, raw, wall, send, recv, loaded):
    chans, bx, by, bz = field.shape
    cx, cy, cz = bx // 2, by // 2, bz // 2
    taps = raw_fine.shape[0]
    place = {axis: lax.axis_index(axis) for axis in ("gx", "gy", "gz")}
    size = dict(zip(("gx", "gy", "gz"), counts))
    axes = ("gx", "gy", "gz")
    gz, nz = place["gz"], size["gz"]
    reach = [(d, 0, 0) for d in (-1, 1, -2, 2)] + [(0, d, 0) for d in (-1, 1, -2, 2)]
    reach += [(a, b, 0) for a in (-1, 1) for b in (-1, 1)] + [(0, 0, -1), (0, 0, 1)]

    def possible(d):
        return all(size[axis] > abs(k) for axis, k in zip(axes, d))

    def has(d):
        found = True
        for axis, k in zip(axes, d):
            if k:
                found = found & (place[axis] + k >= 0) & (place[axis] + k < size[axis])
        return found

    def device(d):
        return tuple(jnp.clip(place[axis] + k, 0, size[axis] - 1) for axis, k in zip(axes, d))

    loads = [
        pltpu.make_async_copy(source, raw.at[k], loaded.at[k])
        for k, source in enumerate((raw_fine, raw_half, raw_quarter, raw_eighth))
    ]
    for load in loads:
        load.start()

    for ref in (uc, u3x, u3y):
        ref[...] = jnp.zeros_like(ref)
    for x in (0, bx + 1):
        u0[x] = jnp.zeros((by + 2, chans, bz), BF16)
    for y in (0, by + 1):
        u0[pl.ds(1, bx), y] = jnp.zeros((bx, chans, bz), BF16)
    for side, d in ((0, -1), (1, 1)):
        @pl.when(jnp.logical_not(has((0, 0, d))))
        def _():
            for ref in (z0, zc, z3):
                ref[side] = jnp.zeros(ref.shape[1:], BF16)

    barrier = pltpu.get_barrier_semaphore()
    for d in reach:
        if possible(d):
            @pl.when(has(d))
            def _():
                pl.semaphore_signal(barrier, inc=1, device_id=device(d), device_id_type=MESH)

    rows = chans * by
    perm_row, perm_col = iota((rows, rows), 0), iota((rows, rows), 1)
    perm = jnp.where(perm_col == (perm_row % chans) * by + perm_row // chans, 1.0, 0.0).astype(BF16)
    back = jnp.where(perm_row == (perm_col % chans) * by + perm_col // chans, 1.0, 0.0).astype(BF16)

    for x in range(bx):
        slab = field[:, x].astype(F32).reshape(rows, bz).astype(BF16)
        u0[1 + x, 1 : 1 + by] = dot(perm, slab).astype(BF16).reshape(by, chans, bz)

    def halve(blocks, matrix):
        stacked = jnp.concatenate(blocks, axis=0)
        summed = jnp.dot(stacked, matrix, precision=lax.Precision.HIGHEST, preferred_element_type=F32)
        rounded = (summed * 0.125).astype(BF16).astype(F32)
        return [rounded[chans * k : chans * (k + 1)] for k in range(len(blocks))]

    def quads(values, wide, high):
        return [
            values[2 * x * high + 2 * y] + values[(2 * x + 1) * high + 2 * y]
            + values[2 * x * high + 2 * y + 1] + values[(2 * x + 1) * high + 2 * y + 1]
            for x in range(wide // 2) for y in range(high // 2)
        ]

    fine = [u0[1 + x, 1 + y].astype(F32) for x in range(bx) for y in range(by)]
    first = halve(quads(fine, bx, by), pair_sum(0, 0, bz))
    second = halve(quads(first, cx, cy), pair_sum(0, cz, bz))
    third = halve(quads(second, cx // 2, cy // 2), pair_sum(cz, 0, bz))
    for x in range(cx):
        for y in range(cy):
            uc[2 + x, 2 + y] = (first[x * cy + y] + second[(x % 2) * (cy // 2) + y % 2]).astype(BF16)
    u3x[2] = third[0].astype(BF16)

    peers = sum(has(d).astype(jnp.int32) for d in reach if possible(d))
    pl.semaphore_wait(barrier, peers)

    made = []

    def copy(d, src, dst):
        k = len(made)
        made.append(d)
        return d, pltpu.make_async_remote_copy(
            src_ref=src, dst_ref=dst, send_sem=send.at[k], recv_sem=recv.at[k],
            device_id=device(d), device_id_type=MESH)

    def start(copies):
        for d, c in copies:
            if possible(d):
                @pl.when(has(d))
                def _():
                    c.start()

    def arrive(copies):
        for d, c in copies:
            if possible(d):
                @pl.when(has(tuple(-k for k in d)))
                def _():
                    c.wait_recv()

    def leave(copies):
        for d, c in copies:
            if possible(d):
                @pl.when(has(d))
                def _():
                    c.wait_send()

    def spans(d, length, depth):
        if d == 0:
            return depth, depth, length
        return (depth, length + depth, depth) if d < 0 else (length, 0, depth)

    def rims(ref, length_x, length_y, depth):
        result = []
        for dx in (-1, 0, 1):
            for dy in (-1, 0, 1):
                if dx or dy:
                    sx, tx, wx = spans(dx, length_x, depth)
                    sy, ty, wy = spans(dy, length_y, depth)
                    result.append(copy((dx, dy, 0), ref.at[pl.ds(sx, wx), pl.ds(sy, wy)],
                                       ref.at[pl.ds(tx, wx), pl.ds(ty, wy)]))
        return result

    def across(ref, dst, pieces):
        return [
            copy((0, 0, d), ref.at[piece], dst.at[((1 - d) // 2,) + piece])
            for d in (-1, 1) for piece in pieces
        ]

    def frame(length_x, length_y, depth):
        whole_y = pl.ds(0, length_y + 2 * depth)
        mid_x = pl.ds(depth, length_x)
        return [
            (pl.ds(0, depth), whole_y), (pl.ds(length_x + depth, depth), whole_y),
            (mid_x, pl.ds(0, depth)), (mid_x, pl.ds(length_y + depth, depth)),
        ]

    x_last = [copy((d, 0, 0), u3x.at[2], u3x.at[2 - d]) for d in (-1, 1, -2, 2)]
    y_last = [copy((0, d, 0), u3y.at[2], u3y.at[2 - d]) for d in (-1, 1, -2, 2)]
    z_last = [copy((0, 0, d), u3y, z3.at[(1 - d) // 2]) for d in (-1, 1)]
    small = rims(uc, cx, cy, 2)
    fine_rims = rims(u0, bx, by, 1)
    z_own = across(uc, zc, [(pl.ds(2, cx), pl.ds(2, cy))])
    z_own_fine = across(u0, z0, [(pl.ds(1, bx), pl.ds(1, by))])
    z_small = across(uc, zc, frame(cx, cy, 2))
    z_fine = across(u0, z0, frame(bx, by, 1))

    start(x_last)
    start(small)
    start(z_own_fine)
    start(z_own)
    start(fine_rims)

    eye = jnp.where(iota((chans, chans), 0) == iota((chans, chans), 1), 1.0, 0.0).astype(BF16)

    def turned(value):
        return lax.dot_general(eye, value, (((1,), (1,)), ((), ())), preferred_element_type=F32).astype(BF16)

    for load in loads:
        load.wait()
    fine_rows = jnp.concatenate([raw[0], turned(mixing[...])], axis=0)
    wall[0] = turned(fine_rows)
    for k in range(1, 4):
        wall[k, :, pl.ds(0, taps)] = turned(raw[k])

    arrive(x_last)
    width = bz // 8
    packed = u3x[0].astype(F32)
    for k in range(1, 5):
        packed = packed + pltpu.roll(u3x[k].astype(F32), k * width, 1)
    u3y[2] = packed.astype(BF16)
    start(y_last)

    lane = iota((chans, bz), 1)

    def roll(value, amount):
        amount = amount % bz
        return value if amount == 0 else pltpu.roll(value, amount, 1)

    def window(own, low, high, offset, length):
        own, low, high = own.astype(F32), low.astype(F32), high.astype(F32)
        value = jnp.where(lane < 2, roll(low, 2 - offset - length), 0.0)
        value = jnp.where((lane >= 2) & (lane < length + 2), roll(own, 2 - offset), value)
        value = jnp.where((lane >= length + 2) & (lane < length + 4), roll(high, length + 2 - offset), value)
        return jnp.concatenate([roll(value, -dz) for dz in range(3)], axis=0).astype(BF16)

    def fill_fine(x, y):
        own = u0[x, y]
        wide = own.astype(F32)
        low = jnp.where(lane == bz - 1, z0[0, x, y].astype(F32), wide)
        high = jnp.where(lane == 0, z0[1, x, y].astype(F32), wide)
        v0[x, y] = jnp.concatenate([roll(low, 1).astype(BF16), own, roll(high, -1).astype(BF16)], axis=0)

    def patches(v, x, y):
        return jnp.concatenate(
            [v[x + dx, pl.ds(y, 3)].reshape(taps // 3, bz) for dx in range(3)], axis=0)

    weights = wall[0]

    def fine_pair(xa, xb, y):
        sides = [jnp.concatenate([patches(v0, x, y), u0[x + 1, y + 1]], axis=0) for x in (xa, xb)]
        value = dot(weights, jnp.concatenate(sides, axis=1))
        y0[xa, y] = value[:, :bz]
        y0[xb, y] = value[:, bz:]

    arrive(z_own_fine)

    def fill_own(x, carry):
        for y in range(by):
            fill_fine(x + 1, y + 1)
        return carry

    lax.fori_loop(0, bx, fill_own, 0)

    arrive(small)
    start(z_small)
    arrive(y_last)
    start(z_last)
    arrive(fine_rims)
    start(z_fine)

    def interior(p, carry):
        for y in range(1, by - 1):
            fine_pair(1 + 2 * p, 2 + 2 * p, y)
        return carry

    lax.fori_loop(0, (bx - 2) // 2, interior, 0)

    arrive(z_own)
    arrive(z_small)
    arrive(z_last)

    for k in range(5):
        for y in range(5):
            v3[k, y] = window(u3y[y], z3[0, y], z3[1, y], k * width, width)

    def fill2(x, carry):
        source_x = jnp.where(x >= 4, x + 2, x)
        for y in range(6):
            sy = y + 2 if y >= 4 else y
            v2[x, y] = window(uc[source_x, sy], zc[0, source_x, sy], zc[1, source_x, sy], cz, cz // 2)
        return carry

    lax.fori_loop(0, 6, fill2, 0)

    def fill1(x, carry):
        for y in range(cy + 4):
            v1[x, y] = window(uc[x, y], zc[0, x, y], zc[1, x, y], 0, cz)
        return carry

    lax.fori_loop(0, cx + 4, fill1, 0)

    def rim(length):
        low = jnp.where(gz > 0, 1.0, 0.0)
        high = jnp.where(gz < nz - 1, 1.0, 0.0)
        inside = jnp.where((lane >= 1) & (lane <= length), 1.0, 0.0)
        return inside + jnp.where(lane == 0, low, 0.0) + jnp.where(lane == length + 1, high, 0.0)

    def inside(index, length, axis):
        low = (index > 0) | (place[axis] > 0)
        high = (index <= length) | (place[axis] < size[axis] - 1)
        return jnp.where(low & high, 1.0, 0.0)

    rim3 = rim(width)
    w3 = wall[3, :, pl.ds(0, taps)]
    for x in range(3):
        for y in range(3):
            value = dot(w3, patches(v3, x, y))
            scale = inside(x, 1, "gx") * inside(y, 1, "gy")
            zz3[x, y] = (value * (rim3 * scale)).astype(BF16)

    def along_y(values, wide, shift):
        result = []
        for f in range(wide):
            cell = f - shift
            main = (cell >> 1) + 1
            other = main + 1 if cell & 1 else main - 1
            result.append(0.75 * values[main] + 0.25 * values[other])
        return result

    def raised(zz, coarse_size, shift):
        count_x, count_y = zz.shape[:2]
        spread_z = spread(coarse_size, shift, bz)
        flat = dot(zz[...].reshape(count_x * count_y * chans, bz), spread_z)
        return flat.reshape(count_x, count_y, chans, bz)

    def level(weights, v, zz, coarse, size_x, size_y, length, qy):
        mask = rim(length)
        for i in range((size_x + 2) // 2):
            for y in range(size_y + 2):
                value = dot(weights, jnp.concatenate(
                    [patches(v, 2 * i, y), patches(v, 2 * i + 1, y)], axis=1))
                a, b = qy[i][y], qy[i + 1][y]
                scale = mask * inside(y, size_y, "gy")
                zz[2 * i, y] = ((value[:, :bz] + 0.75 * a + 0.25 * b)
                                * (scale * inside(2 * i, size_x, "gx"))).astype(BF16)
                zz[2 * i + 1, y] = ((value[:, bz:] + 0.75 * b + 0.25 * a)
                                    * (scale * inside(2 * i + 1, size_x, "gx"))).astype(BF16)

    q3 = raised(zz3, width, 1)
    qy3 = [along_y([q3[x, y] for y in range(3)], 4, 1) for x in range(3)]
    level(wall[2, :, pl.ds(0, taps)], v2, zz2, zz3, cx // 2, cy // 2, cz // 2, qy3)
    q2 = raised(zz2, cz // 2, 1)
    qy2 = [along_y([q2[x, y] for y in range(cy // 2 + 2)], cy + 2, 1) for x in range(cx // 2 + 2)]
    level(wall[1, :, pl.ds(0, taps)], v1, zz1, zz2, cx, cy, cz, qy2)
    q1 = raised(zz1, cz, 0)
    for x in range(cx + 2):
        for y, value in enumerate(along_y([q1[x, y] for y in range(cy + 2)], by, 0)):
            qy0[x, y] = value

    arrive(z_fine)

    def fill_rows(y, carry):
        for x in (0, bx + 1):
            fill_fine(x, y)
        return carry

    lax.fori_loop(0, by + 2, fill_rows, 0)

    def fill_columns(x, carry):
        for y in (0, by + 1):
            fill_fine(x + 1, y)
        return carry

    lax.fori_loop(0, bx, fill_columns, 0)

    for y in range(by):
        fine_pair(0, bx - 1, y)

    def edges(p, carry):
        for y in (0, by - 1):
            fine_pair(1 + 2 * p, 2 + 2 * p, y)
        return carry

    lax.fori_loop(0, (bx - 2) // 2, edges, 0)

    scale = math.sqrt(2.0 / math.pi)

    def finish(i, carry):
        done = []
        for y in range(by):
            a, b, c = qy0[i, y], qy0[i + 1, y], qy0[i + 2, y]
            value = jnp.concatenate(
                [y0[2 * i, y] + (0.75 * b + 0.25 * a), y0[2 * i + 1, y] + (0.75 * b + 0.25 * c)], axis=1)
            inner = scale * (value + 0.044715 * (value * value * value))
            done.append((0.5 * value * (1.0 + jnp.tanh(inner))).astype(BF16))
        whole = dot(back, jnp.concatenate(done, axis=0))
        for k in range(2):
            part = whole[:, k * bz : (k + 1) * bz].reshape(chans, by, bz).astype(BF16)
            out[:, pl.ds(2 * i + k, 1)] = part.reshape(chans, 1, by, bz)
        return carry

    lax.fori_loop(0, bx // 2, finish, 0)

    for group in (x_last, small, z_own_fine, z_own, fine_rims, y_last, z_small, z_last, z_fine):
        leave(group)


def solution(mesh):
    counts = tuple(mesh.shape[axis] for axis in ("gx", "gy", "gz"))

    def on_device(field, mixing, *kernels):
        chans, bx, by, bz = field.shape
        cx, cy = bx // 2, by // 2
        rows = [k.reshape(-1, chans) for k in kernels]
        taps = rows[0].shape[0]
        vmem = pl.BlockSpec(memory_space=pltpu.VMEM)
        anywhere = pl.BlockSpec(memory_space=pl.ANY)

        def buf(*dims, dtype=BF16):
            return pltpu.VMEM(dims, dtype)

        fine = (bx + 2, by + 2, chans, bz)
        coarse = (cx + 4, cy + 4, chans, bz)
        return pl.pallas_call(
            functools.partial(kernel, counts),
            out_shape=jax.ShapeDtypeStruct(field.shape, BF16),
            in_specs=[vmem] * 2 + [anywhere] * 4,
            out_specs=vmem,
            scratch_shapes=[
                buf(*fine), buf(*coarse), buf(5, chans, bz), buf(5, chans, bz),
                buf(2, *fine), buf(2, *coarse), buf(2, 5, chans, bz),
                buf(bx + 2, by + 2, 3 * chans, bz),
                buf(cx + 4, cy + 4, 3 * chans, bz),
                buf(6, 6, 3 * chans, bz), buf(5, 5, 3 * chans, bz),
                buf(cx + 2, cy + 2, chans, bz), buf(4, 4, chans, bz), buf(3, 3, chans, bz),
                buf(cx + 2, by, chans, bz, dtype=F32), buf(bx, by, chans, bz, dtype=F32),
                buf(4, taps, chans), buf(4, chans, taps + chans),
                pltpu.SemaphoreType.DMA((48,)), pltpu.SemaphoreType.DMA((48,)),
                pltpu.SemaphoreType.DMA((4,)),
            ],
            compiler_params=pltpu.CompilerParams(
                collective_id=0, has_side_effects=True, vmem_limit_bytes=24 * 2**20),
        )(field, mixing, *rows)

    placed = (P(None, "gx", "gy", "gz"), P(), P(), P(), P(), P())
    return jax.shard_map(
        on_device, mesh=mesh, in_specs=placed, out_specs=P(None, "gx", "gy", "gz"), check_vma=False
    )
```

```python
import functools
import math

import jax
import jax.numpy as jnp
from jax import lax
from jax.experimental import pallas as pl
from jax.experimental.pallas import tpu as pltpu
from jax.sharding import PartitionSpec as P

F32 = jnp.float32
BF16 = jnp.bfloat16
MESH = pl.DeviceIdType.MESH


def iota(shape, dim):
    return lax.broadcasted_iota(jnp.int32, shape, dim)


def pair_sum(first, offset, lanes):
    source, target = iota((lanes, lanes), 0) - first, iota((lanes, lanes), 1) - offset
    return jnp.where(
        (source >= 0) & (target >= 0) & (lax.shift_right_arithmetic(source, 1) == target), 1.0, 0.0
    )


def spread(coarse_size, fine_shift, lanes):
    coarse = iota((lanes, lanes), 0) - 1
    fine = iota((lanes, lanes), 1) - fine_shift
    main = lax.shift_right_arithmetic(fine, 1)
    other = main + 2 * (fine & 1) - 1
    weight = jnp.where(coarse == main, 0.75, jnp.where(coarse == other, 0.25, 0.0))
    return jnp.where(coarse <= coarse_size, weight, 0.0).astype(BF16)


def dot(a, b):
    return jnp.dot(a, b, preferred_element_type=F32)


def kernel(counts, field_in, mixing_in, raw_fine, raw_half, raw_quarter, raw_eighth, out, u0, uc, u2, u3x, u3y,
           z0, zc, z2, z3, v0, v1, v2, v3, zz1, zz2, zz3, qy0, y0, raw, wall, field, mixing, send, recv, loaded):
    chans, bx, by, bz = field.shape
    cx, cy, cz = bx // 2, by // 2, bz // 2
    taps = raw_fine.shape[0]
    place = {axis: lax.axis_index(axis) for axis in ("gx", "gy", "gz")}
    size = dict(zip(("gx", "gy", "gz"), counts))
    axes = ("gx", "gy", "gz")
    gz, nz = place["gz"], size["gz"]
    reach = [(d, 0, 0) for d in (-1, 1, -2, 2)] + [(0, d, 0) for d in (-1, 1, -2, 2)]
    reach += [(a, b, 0) for a in (-1, 1) for b in (-1, 1)] + [(0, 0, -1), (0, 0, 1)]

    def possible(d):
        return all(size[axis] > abs(k) for axis, k in zip(axes, d))

    def has(d):
        found = True
        for axis, k in zip(axes, d):
            if k:
                found = found & (place[axis] + k >= 0) & (place[axis] + k < size[axis])
        return found

    def device(d):
        return tuple(jnp.clip(place[axis] + k, 0, size[axis] - 1) for axis, k in zip(axes, d))

    loads = [
        pltpu.make_async_copy(source, raw.at[k], loaded.at[k])
        for k, source in enumerate((raw_fine, raw_half, raw_quarter, raw_eighth))
    ]
    loads.append(pltpu.make_async_copy(mixing_in, mixing, loaded.at[4]))
    load_field = pltpu.make_async_copy(field_in, field, loaded.at[5])
    load_field.start()
    for load in loads:
        load.start()

    for ref in (uc, u2, u3x, u3y):
        ref[...] = jnp.zeros_like(ref)
    for x in (0, bx + 1):
        u0[x] = jnp.zeros((by + 2, chans, bz), BF16)
    for y in (0, by + 1):
        u0[pl.ds(1, bx), y] = jnp.zeros((bx, chans, bz), BF16)
    for side, d in ((0, -1), (1, 1)):
        @pl.when(jnp.logical_not(has((0, 0, d))))
        def _():
            for ref in (z0, zc, z2, z3):
                ref[side] = jnp.zeros(ref.shape[1:], BF16)

    barrier = pltpu.get_barrier_semaphore()
    for d in reach:
        if possible(d):
            @pl.when(has(d))
            def _():
                pl.semaphore_signal(barrier, inc=1, device_id=device(d), device_id_type=MESH)

    rows = chans * by
    perm_row, perm_col = iota((rows, rows), 0), iota((rows, rows), 1)
    perm = jnp.where(perm_col == (perm_row % chans) * by + perm_row // chans, 1.0, 0.0).astype(BF16)
    back = jnp.where(perm_row == (perm_col % chans) * by + perm_col // chans, 1.0, 0.0).astype(BF16)

    load_field.wait()
    for x in range(bx):
        slab = field[:, x].astype(F32).reshape(rows, bz).astype(BF16)
        u0[1 + x, 1 : 1 + by] = dot(perm, slab).astype(BF16).reshape(by, chans, bz)

    def halve(blocks, matrix):
        stacked = jnp.concatenate(blocks, axis=0)
        summed = jnp.dot(stacked, matrix, precision=lax.Precision.HIGHEST, preferred_element_type=F32)
        rounded = (summed * 0.125).astype(BF16).astype(F32)
        return [rounded[chans * k : chans * (k + 1)] for k in range(len(blocks))]

    def quads(values, wide, high):
        return [
            values[2 * x * high + 2 * y] + values[(2 * x + 1) * high + 2 * y]
            + values[2 * x * high + 2 * y + 1] + values[(2 * x + 1) * high + 2 * y + 1]
            for x in range(wide // 2) for y in range(high // 2)
        ]

    fine = [u0[1 + x, 1 + y].astype(F32) for x in range(bx) for y in range(by)]
    first = halve(quads(fine, bx, by), pair_sum(0, 0, bz))
    second = halve(quads(first, cx, cy), pair_sum(0, 0, bz))
    third = halve(quads(second, cx // 2, cy // 2), pair_sum(0, 0, bz))
    for x in range(cx // 2):
        for y in range(cy):
            pair = first[2 * x * cy + y] + pltpu.roll(first[(2 * x + 1) * cy + y], cz, 1)
            uc[1 + x, 2 + y] = pair.astype(BF16)
    block = second[0]
    for k in range(1, 4):
        block = block + pltpu.roll(second[k], k * (cz // 2), 1)
    u2[1, 1] = block.astype(BF16)
    u3x[2] = third[0].astype(BF16)

    peers = sum(has(d).astype(jnp.int32) for d in reach if possible(d))
    pl.semaphore_wait(barrier, peers)

    made = []

    def copy(d, src, dst):
        k = len(made)
        made.append(d)
        return d, pltpu.make_async_remote_copy(
            src_ref=src, dst_ref=dst, send_sem=send.at[k], recv_sem=recv.at[k],
            device_id=device(d), device_id_type=MESH)

    def start(copies):
        for d, c in copies:
            if possible(d):
                @pl.when(has(d))
                def _():
                    c.start()

    def arrive(copies):
        for d, c in copies:
            if possible(d):
                @pl.when(has(tuple(-k for k in d)))
                def _():
                    c.wait_recv()

    def leave(copies):
        for d, c in copies:
            if possible(d):
                @pl.when(has(d))
                def _():
                    c.wait_send()

    def spans(d, length, depth):
        if d == 0:
            return depth, depth, length
        return (depth, length + depth, depth) if d < 0 else (length, 0, depth)

    around = [(dx, dy) for dx in (-1, 0, 1) for dy in (-1, 0, 1) if dx or dy]

    def rims(ref, length_x, length_y, depth_x, depth_y):
        result = []
        for dx, dy in around:
            sx, tx, wx = spans(dx, length_x, depth_x)
            sy, ty, wy = spans(dy, length_y, depth_y)
            result.append(copy((dx, dy, 0), ref.at[pl.ds(sx, wx), pl.ds(sy, wy)],
                               ref.at[pl.ds(tx, wx), pl.ds(ty, wy)]))
        return result

    def across(ref, dst, pieces):
        return [
            copy((0, 0, d), ref.at[piece], dst.at[((1 - d) // 2,) + piece])
            for d in (-1, 1) for piece in pieces
        ]

    def frame(length_x, length_y, depth_x, depth_y):
        whole_y = pl.ds(0, length_y + 2 * depth_y)
        mid_x = pl.ds(depth_x, length_x)
        return [
            (pl.ds(0, depth_x), whole_y), (pl.ds(length_x + depth_x, depth_x), whole_y),
            (mid_x, pl.ds(0, depth_y)), (mid_x, pl.ds(length_y + depth_y, depth_y)),
        ]

    x_last = [copy((d, 0, 0), u3x.at[2], u3x.at[2 - d]) for d in (-1, 1, -2, 2)]
    y_last = [copy((0, d, 0), u3y.at[2], u3y.at[2 - d]) for d in (-1, 1, -2, 2)]
    z_last = [copy((0, 0, d), u3y, z3.at[(1 - d) // 2]) for d in (-1, 1)]
    small = rims(uc, cx // 2, cy, 1, 2)
    small += [copy((dx, dy, 0), u2.at[1, 1], u2.at[1 - dx, 1 - dy]) for dx, dy in around]
    fine_rims = rims(u0, bx, by, 1, 1)
    z_own = across(uc, zc, [(pl.ds(1, cx // 2), pl.ds(2, cy))])
    z_own_fine = across(u0, z0, [(pl.ds(1, bx), pl.ds(1, by))])
    z_small = across(uc, zc, frame(cx // 2, cy, 1, 2))
    z_small += [copy((0, 0, d), u2, z2.at[(1 - d) // 2]) for d in (-1, 1)]
    z_fine = across(u0, z0, frame(bx, by, 1, 1))

    start(x_last)
    start(small)
    start(z_own_fine)
    start(z_own)
    start(fine_rims)

    eye = jnp.where(iota((chans, chans), 0) == iota((chans, chans), 1), 1.0, 0.0).astype(BF16)

    def turned(value):
        return lax.dot_general(eye, value, (((1,), (1,)), ((), ())), preferred_element_type=F32).astype(BF16)

    for load in loads:
        load.wait()
    fine_rows = jnp.concatenate([raw[0], turned(mixing[...])], axis=0)
    wall[0] = turned(fine_rows)
    for k in range(1, 4):
        wall[k, :, pl.ds(0, taps)] = turned(raw[k])

    arrive(x_last)
    width = bz // 8
    packed = u3x[0].astype(F32)
    for k in range(1, 5):
        packed = packed + pltpu.roll(u3x[k].astype(F32), k * width, 1)
    u3y[2] = packed.astype(BF16)
    start(y_last)

    lane = iota((chans, bz), 1)

    def roll(value, amount):
        amount = amount % bz
        return value if amount == 0 else pltpu.roll(value, amount, 1)

    def window(own, low, high, offset, length):
        own, low, high = own.astype(F32), low.astype(F32), high.astype(F32)
        value = jnp.where(lane < 2, roll(low, 2 - offset - length), 0.0)
        value = jnp.where((lane >= 2) & (lane < length + 2), roll(own, 2 - offset), value)
        value = jnp.where((lane >= length + 2) & (lane < length + 4), roll(high, length + 2 - offset), value)
        return jnp.concatenate([roll(value, -dz) for dz in range(3)], axis=0).astype(BF16)

    def fill_fine(x, y):
        own = u0[x, y]
        wide = own.astype(F32)
        low = jnp.where(lane == bz - 1, z0[0, x, y].astype(F32), wide)
        high = jnp.where(lane == 0, z0[1, x, y].astype(F32), wide)
        v0[x, y] = jnp.concatenate([roll(low, 1).astype(BF16), own, roll(high, -1).astype(BF16)], axis=0)

    def patches(v, x, y):
        return jnp.concatenate(
            [v[x + dx, pl.ds(y, 3)].reshape(taps // 3, bz) for dx in range(3)], axis=0)

    weights = wall[0]

    def fine_pair(xa, xb, y):
        sides = [jnp.concatenate([patches(v0, x, y), u0[x + 1, y + 1]], axis=0) for x in (xa, xb)]
        value = dot(weights, jnp.concatenate(sides, axis=1))
        y0[xa, y] = value[:, :bz]
        y0[xb, y] = value[:, bz:]

    arrive(z_own_fine)

    def fill_own(x, carry):
        for y in range(by):
            fill_fine(x + 1, y + 1)
        return carry

    lax.fori_loop(0, bx, fill_own, 0)

    def interior(p, carry):
        for y in range(1, by - 1):
            fine_pair(1 + 2 * p, 2 + 2 * p, y)
        return carry

    lax.fori_loop(0, (bx - 2) // 2, interior, 0)

    arrive(y_last)
    start(z_last)
    arrive(small)
    start(z_small)
    arrive(z_own)
    arrive(z_last)

    for k in range(5):
        for y in range(5):
            v3[k, y] = window(u3y[y], z3[0, y], z3[1, y], k * width, width)

    def rim(length):
        low = jnp.where(gz > 0, 1.0, 0.0)
        high = jnp.where(gz < nz - 1, 1.0, 0.0)
        inside = jnp.where((lane >= 1) & (lane <= length), 1.0, 0.0)
        return inside + jnp.where(lane == 0, low, 0.0) + jnp.where(lane == length + 1, high, 0.0)

    def inside(index, length, axis):
        low = (index > 0) | (place[axis] > 0)
        high = (index <= length) | (place[axis] < size[axis] - 1)
        return jnp.where(low & high, 1.0, 0.0)

    rim3 = rim(width)
    w3 = wall[3, :, pl.ds(0, taps)]
    for x in range(3):
        for y in range(3):
            value = dot(w3, patches(v3, x, y))
            scale = inside(x, 1, "gx") * inside(y, 1, "gy")
            zz3[x, y] = (value * (rim3 * scale)).astype(BF16)

    def along_y(values, wide, shift):
        result = []
        for f in range(wide):
            cell = f - shift
            main = (cell >> 1) + 1
            other = main + 1 if cell & 1 else main - 1
            result.append(0.75 * values[main] + 0.25 * values[other])
        return result

    def raised(zz, coarse_size, shift):
        count_x, count_y = zz.shape[:2]
        spread_z = spread(coarse_size, shift, bz)
        flat = dot(zz[...].reshape(count_x * count_y * chans, bz), spread_z)
        return flat.reshape(count_x, count_y, chans, bz)

    def level(weights, v, zz, coarse, size_x, size_y, length, qy):
        mask = rim(length)
        for i in range((size_x + 2) // 2):
            for y in range(size_y + 2):
                value = dot(weights, jnp.concatenate(
                    [patches(v, 2 * i, y), patches(v, 2 * i + 1, y)], axis=1))
                a, b = qy[i][y], qy[i + 1][y]
                scale = mask * inside(y, size_y, "gy")
                zz[2 * i, y] = ((value[:, :bz] + 0.75 * a + 0.25 * b)
                                * (scale * inside(2 * i, size_x, "gx"))).astype(BF16)
                zz[2 * i + 1, y] = ((value[:, bz:] + 0.75 * b + 0.25 * a)
                                    * (scale * inside(2 * i + 1, size_x, "gx"))).astype(BF16)

    arrive(z_small)

    def fill2(x, carry):
        for k in range(2):
            for y in range(6):
                offset = (2 * k + y % 2) * (cz // 2)
                v2[2 * x + k, y] = window(
                    u2[x, y // 2], z2[0, x, y // 2], z2[1, x, y // 2], offset, cz // 2)
        return carry

    lax.fori_loop(0, 3, fill2, 0)

    def fill1(x, carry):
        for y in range(cy + 4):
            own, low, high = uc[x, y], zc[0, x, y], zc[1, x, y]
            for k in range(2):
                v1[2 * x + k, y] = window(own, low, high, k * cz, cz)
        return carry

    lax.fori_loop(0, cx // 2 + 2, fill1, 0)

    q3 = raised(zz3, width, 1)
    qy3 = [along_y([q3[x, y] for y in range(3)], 4, 1) for x in range(3)]
    level(wall[2, :, pl.ds(0, taps)], v2, zz2, zz3, cx // 2, cy // 2, cz // 2, qy3)
    arrive(fine_rims)
    start(z_fine)

    q2 = raised(zz2, cz // 2, 1)
    qy2 = [along_y([q2[x, y] for y in range(cy // 2 + 2)], cy + 2, 1) for x in range(cx // 2 + 2)]
    level(wall[1, :, pl.ds(0, taps)], v1, zz1, zz2, cx, cy, cz, qy2)
    q1 = raised(zz1, cz, 0)
    for x in range(cx + 2):
        for y, value in enumerate(along_y([q1[x, y] for y in range(cy + 2)], by, 0)):
            qy0[x, y] = value

    arrive(z_fine)

    def fill_rows(y, carry):
        for x in (0, bx + 1):
            fill_fine(x, y)
        return carry

    lax.fori_loop(0, by + 2, fill_rows, 0)

    def fill_columns(x, carry):
        for y in (0, by + 1):
            fill_fine(x + 1, y)
        return carry

    lax.fori_loop(0, bx, fill_columns, 0)

    for y in range(by):
        fine_pair(0, bx - 1, y)

    def edges(p, carry):
        for y in (0, by - 1):
            fine_pair(1 + 2 * p, 2 + 2 * p, y)
        return carry

    lax.fori_loop(0, (bx - 2) // 2, edges, 0)

    scale = math.sqrt(2.0 / math.pi)

    def finish(i, carry):
        done = []
        for y in range(by):
            a, b, c = qy0[i, y], qy0[i + 1, y], qy0[i + 2, y]
            value = jnp.concatenate(
                [y0[2 * i, y] + (0.75 * b + 0.25 * a), y0[2 * i + 1, y] + (0.75 * b + 0.25 * c)], axis=1)
            inner = scale * (value + 0.044715 * (value * value * value))
            done.append((0.5 * value * (1.0 + jnp.tanh(inner))).astype(BF16))
        whole = dot(back, jnp.concatenate(done, axis=0))
        for k in range(2):
            part = whole[:, k * bz : (k + 1) * bz].reshape(chans, by, bz).astype(BF16)
            out[:, pl.ds(2 * i + k, 1)] = part.reshape(chans, 1, by, bz)
        return carry

    lax.fori_loop(0, bx // 2, finish, 0)

    for group in (x_last, small, z_own_fine, z_own, fine_rims, y_last, z_small, z_last, z_fine):
        leave(group)


def solution(mesh):
    counts = tuple(mesh.shape[axis] for axis in ("gx", "gy", "gz"))

    def on_device(field, mixing, *kernels):
        chans, bx, by, bz = field.shape
        cx, cy = bx // 2, by // 2
        rows = [k.reshape(-1, chans) for k in kernels]
        taps = rows[0].shape[0]
        vmem = pl.BlockSpec(memory_space=pltpu.VMEM)
        remote = pl.BlockSpec(memory_space=pltpu.HBM)

        def buf(*dims, dtype=BF16):
            return pltpu.VMEM(dims, dtype)

        fine = (bx + 2, by + 2, chans, bz)
        coarse = (cx // 2 + 2, cy + 4, chans, bz)
        return pl.pallas_call(
            functools.partial(kernel, counts),
            out_shape=jax.ShapeDtypeStruct(field.shape, BF16),
            in_specs=[remote] * 6,
            out_specs=vmem,
            scratch_shapes=[
                buf(*fine), buf(*coarse), buf(3, 3, chans, bz), buf(5, chans, bz), buf(5, chans, bz),
                buf(2, *fine), buf(2, *coarse), buf(2, 3, 3, chans, bz), buf(2, 5, chans, bz),
                buf(bx + 2, by + 2, 3 * chans, bz),
                buf(cx + 4, cy + 4, 3 * chans, bz),
                buf(6, 6, 3 * chans, bz), buf(5, 5, 3 * chans, bz),
                buf(cx + 2, cy + 2, chans, bz), buf(4, 4, chans, bz), buf(3, 3, chans, bz),
                buf(cx + 2, by, chans, bz, dtype=F32), buf(bx, by, chans, bz, dtype=F32),
                buf(4, taps, chans), buf(4, chans, taps + chans),
                buf(*field.shape), buf(*mixing.shape),
                pltpu.SemaphoreType.DMA((64,)), pltpu.SemaphoreType.DMA((64,)),
                pltpu.SemaphoreType.DMA((6,)),
            ],
            compiler_params=pltpu.CompilerParams(
                collective_id=0, has_side_effects=True, vmem_limit_bytes=56 * 2**20),
        )(field, mixing, *rows)

    placed = (P(None, "gx", "gy", "gz"), P(), P(), P(), P(), P())
    return jax.shard_map(
        on_device, mesh=mesh, in_specs=placed, out_specs=P(None, "gx", "gy", "gz"), check_vma=False
    )
```

```python
import functools
import math

import jax
import jax.numpy as jnp
from jax import lax
from jax.experimental import pallas as pl
from jax.experimental.pallas import tpu as pltpu
from jax.sharding import PartitionSpec as P

F32 = jnp.float32
BF16 = jnp.bfloat16
MESH = pl.DeviceIdType.MESH


def iota(shape, dim):
    return lax.broadcasted_iota(jnp.int32, shape, dim)


def pair_sum(first, offset, lanes):
    source, target = iota((lanes, lanes), 0) - first, iota((lanes, lanes), 1) - offset
    return jnp.where(
        (source >= 0) & (target >= 0) & (lax.shift_right_arithmetic(source, 1) == target), 1.0, 0.0
    )


def spread(coarse_size, fine_shift, lanes):
    coarse = iota((lanes, lanes), 0) - 1
    fine = iota((lanes, lanes), 1) - fine_shift
    main = lax.shift_right_arithmetic(fine, 1)
    other = main + 2 * (fine & 1) - 1
    weight = jnp.where(coarse == main, 0.75, jnp.where(coarse == other, 0.25, 0.0))
    return jnp.where(coarse <= coarse_size, weight, 0.0).astype(BF16)


def dot(a, b):
    return jnp.dot(a, b, preferred_element_type=F32)


def kernel(counts, field_in, mixing_in, raw_fine, raw_half, raw_quarter, raw_eighth, out, u0, uc, u2, u3x, u3y,
           z0, zc, z2, z3, v0, v1, v2, v3, zz1, zz2, zz3, qy0, y0, raw, wall, field, mixing, send, recv, loaded):
    chans, bx, by, bz = field.shape
    cx, cy, cz = bx // 2, by // 2, bz // 2
    taps = raw_fine.shape[0]
    place = {axis: lax.axis_index(axis) for axis in ("gx", "gy", "gz")}
    size = dict(zip(("gx", "gy", "gz"), counts))
    axes = ("gx", "gy", "gz")
    gz, nz = place["gz"], size["gz"]
    reach = [(d, 0, 0) for d in (-1, 1, -2, 2)] + [(0, d, 0) for d in (-1, 1, -2, 2)]
    reach += [(a, b, 0) for a in (-1, 1) for b in (-1, 1)] + [(0, 0, -1), (0, 0, 1)]

    def possible(d):
        return all(size[axis] > abs(k) for axis, k in zip(axes, d))

    def has(d):
        found = True
        for axis, k in zip(axes, d):
            if k:
                found = found & (place[axis] + k >= 0) & (place[axis] + k < size[axis])
        return found

    def device(d):
        return tuple(jnp.clip(place[axis] + k, 0, size[axis] - 1) for axis, k in zip(axes, d))

    loads = [
        pltpu.make_async_copy(source, raw.at[k], loaded.at[k])
        for k, source in enumerate((raw_fine, raw_half, raw_quarter, raw_eighth))
    ]
    loads.append(pltpu.make_async_copy(mixing_in, mixing, loaded.at[4]))
    load_field = pltpu.make_async_copy(field_in, field, loaded.at[5])
    load_field.start()
    for load in loads:
        load.start()

    for ref in (uc, u2, u3x, u3y):
        ref[...] = jnp.zeros_like(ref)
    for x in (0, bx + 1):
        u0[x] = jnp.zeros((by + 2, chans, bz), BF16)
    for y in (0, by + 1):
        u0[pl.ds(1, bx), y] = jnp.zeros((bx, chans, bz), BF16)
    for side, d in ((0, -1), (1, 1)):
        @pl.when(jnp.logical_not(has((0, 0, d))))
        def _():
            for ref in (z0, zc, z2, z3):
                ref[side] = jnp.zeros(ref.shape[1:], BF16)

    barrier = pltpu.get_barrier_semaphore()
    for d in reach:
        if possible(d):
            @pl.when(has(d))
            def _():
                pl.semaphore_signal(barrier, inc=1, device_id=device(d), device_id_type=MESH)

    rows = chans * by
    perm_row, perm_col = iota((rows, rows), 0), iota((rows, rows), 1)
    perm = jnp.where(perm_col == (perm_row % chans) * by + perm_row // chans, 1.0, 0.0).astype(BF16)
    back = jnp.where(perm_row == (perm_col % chans) * by + perm_col // chans, 1.0, 0.0).astype(BF16)

    load_field.wait()
    for x in range(bx):
        slab = field[:, x].astype(F32).reshape(rows, bz).astype(BF16)
        u0[1 + x, 1 : 1 + by] = dot(perm, slab).astype(BF16).reshape(by, chans, bz)

    def halve(blocks, matrix):
        stacked = jnp.concatenate(blocks, axis=0)
        summed = jnp.dot(stacked, matrix, precision=lax.Precision.HIGHEST, preferred_element_type=F32)
        rounded = (summed * 0.125).astype(BF16).astype(F32)
        return [rounded[chans * k : chans * (k + 1)] for k in range(len(blocks))]

    def quads(values, wide, high):
        return [
            values[2 * x * high + 2 * y] + values[(2 * x + 1) * high + 2 * y]
            + values[2 * x * high + 2 * y + 1] + values[(2 * x + 1) * high + 2 * y + 1]
            for x in range(wide // 2) for y in range(high // 2)
        ]

    fine = [u0[1 + x, 1 + y].astype(F32) for x in range(bx) for y in range(by)]
    first = halve(quads(fine, bx, by), pair_sum(0, 0, bz))
    second = halve(quads(first, cx, cy), pair_sum(0, 0, bz))
    third = halve(quads(second, cx // 2, cy // 2), pair_sum(0, 0, bz))
    for x in range(cx // 2):
        for y in range(cy):
            pair = first[2 * x * cy + y] + pltpu.roll(first[(2 * x + 1) * cy + y], cz, 1)
            uc[1 + x, 2 + y] = pair.astype(BF16)
    block = second[0]
    for k in range(1, 4):
        block = block + pltpu.roll(second[k], k * (cz // 2), 1)
    u2[1, 1] = block.astype(BF16)
    u3x[2] = third[0].astype(BF16)

    peers = sum(has(d).astype(jnp.int32) for d in reach if possible(d))
    pl.semaphore_wait(barrier, peers)

    made = []

    def copy(d, src, dst):
        k = len(made)
        made.append(d)
        return d, pltpu.make_async_remote_copy(
            src_ref=src, dst_ref=dst, send_sem=send.at[k], recv_sem=recv.at[k],
            device_id=device(d), device_id_type=MESH)

    def start(copies):
        for d, c in copies:
            if possible(d):
                @pl.when(has(d))
                def _():
                    c.start()

    def arrive(copies):
        for d, c in copies:
            if possible(d):
                @pl.when(has(tuple(-k for k in d)))
                def _():
                    c.wait_recv()

    def leave(copies):
        for d, c in copies:
            if possible(d):
                @pl.when(has(d))
                def _():
                    c.wait_send()

    def spans(d, length, depth):
        if d == 0:
            return depth, depth, length
        return (depth, length + depth, depth) if d < 0 else (length, 0, depth)

    around = [(dx, dy) for dx in (-1, 0, 1) for dy in (-1, 0, 1) if dx or dy]

    def rims(ref, length_x, length_y, depth_x, depth_y):
        result = []
        for dx, dy in around:
            sx, tx, wx = spans(dx, length_x, depth_x)
            sy, ty, wy = spans(dy, length_y, depth_y)
            result.append(copy((dx, dy, 0), ref.at[pl.ds(sx, wx), pl.ds(sy, wy)],
                               ref.at[pl.ds(tx, wx), pl.ds(ty, wy)]))
        return result

    def across(ref, dst, pieces):
        return [
            copy((0, 0, d), ref.at[piece], dst.at[((1 - d) // 2,) + piece])
            for d in (-1, 1) for piece in pieces
        ]

    def frame(length_x, length_y, depth_x, depth_y):
        whole_y = pl.ds(0, length_y + 2 * depth_y)
        mid_x = pl.ds(depth_x, length_x)
        return [
            (pl.ds(0, depth_x), whole_y), (pl.ds(length_x + depth_x, depth_x), whole_y),
            (mid_x, pl.ds(0, depth_y)), (mid_x, pl.ds(length_y + depth_y, depth_y)),
        ]

    x_last = [copy((d, 0, 0), u3x.at[2], u3x.at[2 - d]) for d in (-1, 1, -2, 2)]
    y_last = [copy((0, d, 0), u3y.at[2], u3y.at[2 - d]) for d in (-1, 1, -2, 2)]
    z_last = [copy((0, 0, d), u3y, z3.at[(1 - d) // 2]) for d in (-1, 1)]
    small = rims(uc, cx // 2, cy, 1, 2)
    small += [copy((dx, dy, 0), u2.at[1, 1], u2.at[1 - dx, 1 - dy]) for dx, dy in around]
    fine_rims = rims(u0, bx, by, 1, 1)
    z_own = across(uc, zc, [(pl.ds(1, cx // 2), pl.ds(2, cy))])
    z_own_fine = across(u0, z0, [(pl.ds(1, bx), pl.ds(1, by))])
    z_small = across(uc, zc, frame(cx // 2, cy, 1, 2))
    z_small += [copy((0, 0, d), u2, z2.at[(1 - d) // 2]) for d in (-1, 1)]
    z_fine = across(u0, z0, frame(bx, by, 1, 1))

    start(x_last)
    start(small)
    start(z_own_fine)
    start(z_own)
    start(fine_rims)

    eye = jnp.where(iota((chans, chans), 0) == iota((chans, chans), 1), 1.0, 0.0).astype(BF16)

    def turned(value):
        return lax.dot_general(eye, value, (((1,), (1,)), ((), ())), preferred_element_type=F32).astype(BF16)

    for load in loads:
        load.wait()
    fine_rows = jnp.concatenate([raw[0], turned(mixing[...])], axis=0)
    wall[0] = turned(fine_rows)
    for k in range(1, 4):
        wall[k, :, pl.ds(0, taps)] = turned(raw[k])

    arrive(x_last)
    width = bz // 8
    packed = u3x[0].astype(F32)
    for k in range(1, 5):
        packed = packed + pltpu.roll(u3x[k].astype(F32), k * width, 1)
    u3y[2] = packed.astype(BF16)
    start(y_last)

    lane = iota((chans, bz), 1)

    def roll(value, amount):
        amount = amount % bz
        return value if amount == 0 else pltpu.roll(value, amount, 1)

    def window(own, low, high, offset, length):
        edge = (lane < 2) | ((lane >= length + 2) & (lane < length + 4))
        if 2 * length % bz == 0:
            outer = roll(jnp.where(lane >= offset + 2, low, high), 2 - offset - length)
        else:
            outer = jnp.where(lane < 2, roll(low, 2 - offset - length), roll(high, length + 2 - offset))
        zero = jnp.zeros_like(own)
        value = jnp.where(lane < length + 4, jnp.where(edge, outer, roll(own, 2 - offset)), zero)
        return jnp.concatenate([roll(value, -dz) for dz in range(3)], axis=0)

    def fill_fine(x, y):
        own = u0[x, y]
        low = jnp.where(lane == bz - 1, z0[0, x, y], own)
        high = jnp.where(lane == 0, z0[1, x, y], own)
        v0[x, y] = jnp.concatenate([roll(low, 1), own, roll(high, -1)], axis=0)

    def patches(v, x, y):
        return jnp.concatenate(
            [v[x + dx, pl.ds(y, 3)].reshape(taps // 3, bz) for dx in range(3)], axis=0)

    weights = wall[0]

    def fine_pair(xa, xb, y):
        sides = [jnp.concatenate([patches(v0, x, y), u0[x + 1, y + 1]], axis=0) for x in (xa, xb)]
        value = dot(weights, jnp.concatenate(sides, axis=1))
        y0[xa, y] = value[:, :bz]
        y0[xb, y] = value[:, bz:]

    arrive(z_own_fine)

    def fill_own(x, carry):
        for y in range(by):
            fill_fine(x + 1, y + 1)
        return carry

    lax.fori_loop(0, bx, fill_own, 0)

    def interior(p, carry):
        for y in range(1, by - 1):
            fine_pair(1 + 2 * p, 2 + 2 * p, y)
        return carry

    lax.fori_loop(0, (bx - 2) // 2, interior, 0)

    arrive(y_last)
    start(z_last)
    arrive(small)
    start(z_small)
    arrive(z_own)
    arrive(z_last)

    for k in range(5):
        for y in range(5):
            v3[k, y] = window(u3y[y], z3[0, y], z3[1, y], k * width, width)

    def rim(length):
        low = jnp.where(gz > 0, 1.0, 0.0)
        high = jnp.where(gz < nz - 1, 1.0, 0.0)
        inside = jnp.where((lane >= 1) & (lane <= length), 1.0, 0.0)
        return inside + jnp.where(lane == 0, low, 0.0) + jnp.where(lane == length + 1, high, 0.0)

    def inside(index, length, axis):
        low = (index > 0) | (place[axis] > 0)
        high = (index <= length) | (place[axis] < size[axis] - 1)
        return jnp.where(low & high, 1.0, 0.0)

    rim3 = rim(width)
    w3 = wall[3, :, pl.ds(0, taps)]
    for x in range(3):
        for y in range(3):
            value = dot(w3, patches(v3, x, y))
            scale = inside(x, 1, "gx") * inside(y, 1, "gy")
            zz3[x, y] = (value * (rim3 * scale)).astype(BF16)

    def along_y(values, wide, shift):
        result = []
        for f in range(wide):
            cell = f - shift
            main = (cell >> 1) + 1
            other = main + 1 if cell & 1 else main - 1
            result.append(0.75 * values[main] + 0.25 * values[other])
        return result

    def raised(zz, coarse_size, shift):
        count_x, count_y = zz.shape[:2]
        spread_z = spread(coarse_size, shift, bz)
        flat = dot(zz[...].reshape(count_x * count_y * chans, bz), spread_z)
        return flat.reshape(count_x, count_y, chans, bz)

    def level(weights, v, zz, coarse, size_x, size_y, length, qy):
        mask = rim(length)
        for i in range((size_x + 2) // 2):
            for y in range(size_y + 2):
                value = dot(weights, jnp.concatenate(
                    [patches(v, 2 * i, y), patches(v, 2 * i + 1, y)], axis=1))
                a, b = qy[i][y], qy[i + 1][y]
                scale = mask * inside(y, size_y, "gy")
                zz[2 * i, y] = ((value[:, :bz] + 0.75 * a + 0.25 * b)
                                * (scale * inside(2 * i, size_x, "gx"))).astype(BF16)
                zz[2 * i + 1, y] = ((value[:, bz:] + 0.75 * b + 0.25 * a)
                                    * (scale * inside(2 * i + 1, size_x, "gx"))).astype(BF16)

    arrive(z_small)

    def fill2(x, carry):
        for k in range(2):
            for y in range(6):
                offset = (2 * k + y % 2) * (cz // 2)
                v2[2 * x + k, y] = window(
                    u2[x, y // 2], z2[0, x, y // 2], z2[1, x, y // 2], offset, cz // 2)
        return carry

    lax.fori_loop(0, 3, fill2, 0)

    def fill1(x, carry):
        for y in range(cy + 4):
            own, low, high = uc[x, y], zc[0, x, y], zc[1, x, y]
            for k in range(2):
                v1[2 * x + k, y] = window(own, low, high, k * cz, cz)
        return carry

    lax.fori_loop(0, cx // 2 + 2, fill1, 0)

    q3 = raised(zz3, width, 1)
    qy3 = [along_y([q3[x, y] for y in range(3)], 4, 1) for x in range(3)]
    level(wall[2, :, pl.ds(0, taps)], v2, zz2, zz3, cx // 2, cy // 2, cz // 2, qy3)
    arrive(fine_rims)
    start(z_fine)

    q2 = raised(zz2, cz // 2, 1)
    qy2 = [along_y([q2[x, y] for y in range(cy // 2 + 2)], cy + 2, 1) for x in range(cx // 2 + 2)]
    level(wall[1, :, pl.ds(0, taps)], v1, zz1, zz2, cx, cy, cz, qy2)
    q1 = raised(zz1, cz, 0)
    for x in range(cx + 2):
        for y, value in enumerate(along_y([q1[x, y] for y in range(cy + 2)], by, 0)):
            qy0[x, y] = value

    arrive(z_fine)

    def fill_rows(y, carry):
        for x in (0, bx + 1):
            fill_fine(x, y)
        return carry

    lax.fori_loop(0, by + 2, fill_rows, 0)

    def fill_columns(x, carry):
        for y in (0, by + 1):
            fill_fine(x + 1, y)
        return carry

    lax.fori_loop(0, bx, fill_columns, 0)

    for y in range(by):
        fine_pair(0, bx - 1, y)

    def edges(p, carry):
        for y in (0, by - 1):
            fine_pair(1 + 2 * p, 2 + 2 * p, y)
        return carry

    lax.fori_loop(0, (bx - 2) // 2, edges, 0)

    scale = math.sqrt(2.0 / math.pi)

    def finish(i, carry):
        done = []
        for y in range(by):
            a, b, c = qy0[i, y], qy0[i + 1, y], qy0[i + 2, y]
            value = jnp.concatenate(
                [y0[2 * i, y] + (0.75 * b + 0.25 * a), y0[2 * i + 1, y] + (0.75 * b + 0.25 * c)], axis=1)
            inner = scale * (value + 0.044715 * (value * value * value))
            done.append((0.5 * value * (1.0 + jnp.tanh(inner))).astype(BF16))
        whole = dot(back, jnp.concatenate(done, axis=0))
        for k in range(2):
            part = whole[:, k * bz : (k + 1) * bz].reshape(chans, by, bz).astype(BF16)
            out[:, pl.ds(2 * i + k, 1)] = part.reshape(chans, 1, by, bz)
        return carry

    lax.fori_loop(0, bx // 2, finish, 0)

    for group in (x_last, small, z_own_fine, z_own, fine_rims, y_last, z_small, z_last, z_fine):
        leave(group)


def solution(mesh):
    counts = tuple(mesh.shape[axis] for axis in ("gx", "gy", "gz"))

    def on_device(field, mixing, *kernels):
        chans, bx, by, bz = field.shape
        cx, cy = bx // 2, by // 2
        rows = [k.reshape(-1, chans) for k in kernels]
        taps = rows[0].shape[0]
        vmem = pl.BlockSpec(memory_space=pltpu.VMEM)
        remote = pl.BlockSpec(memory_space=pltpu.HBM)

        def buf(*dims, dtype=BF16):
            return pltpu.VMEM(dims, dtype)

        fine = (bx + 2, by + 2, chans, bz)
        coarse = (cx // 2 + 2, cy + 4, chans, bz)
        return pl.pallas_call(
            functools.partial(kernel, counts),
            out_shape=jax.ShapeDtypeStruct(field.shape, BF16),
            in_specs=[remote] * 6,
            out_specs=vmem,
            scratch_shapes=[
                buf(*fine), buf(*coarse), buf(3, 3, chans, bz), buf(5, chans, bz), buf(5, chans, bz),
                buf(2, *fine), buf(2, *coarse), buf(2, 3, 3, chans, bz), buf(2, 5, chans, bz),
                buf(bx + 2, by + 2, 3 * chans, bz),
                buf(cx + 4, cy + 4, 3 * chans, bz),
                buf(6, 6, 3 * chans, bz), buf(5, 5, 3 * chans, bz),
                buf(cx + 2, cy + 2, chans, bz), buf(4, 4, chans, bz), buf(3, 3, chans, bz),
                buf(cx + 2, by, chans, bz, dtype=F32), buf(bx, by, chans, bz, dtype=F32),
                buf(4, taps, chans), buf(4, chans, taps + chans),
                buf(*field.shape), buf(*mixing.shape),
                pltpu.SemaphoreType.DMA((64,)), pltpu.SemaphoreType.DMA((64,)),
                pltpu.SemaphoreType.DMA((6,)),
            ],
            compiler_params=pltpu.CompilerParams(
                collective_id=0, has_side_effects=True, vmem_limit_bytes=56 * 2**20),
        )(field, mixing, *rows)

    placed = (P(None, "gx", "gy", "gz"), P(), P(), P(), P(), P())
    return jax.shard_map(
        on_device, mesh=mesh, in_specs=placed, out_specs=P(None, "gx", "gy", "gz"), check_vma=False
    )
```
